64 devices in a mesh: data: 4 (over x, y), ep: 16 (over z, core).
Axes of the slice: x: 2, y: 2, z: 8, core: 2. Of those that a mesh axis runs over, the one named last changes fastest.
The devices are a block of a 4x4x8 slice.
Arguments:
- x_in: bfloat16 [64, 384, 2048], P(('data', 'ep')), parts along dimension 0
- w_query: bfloat16 [2048, 16, 128], P('ep')
- w_keyval: bfloat16 [2048, 8, 128], P('ep')
- w_out: bfloat16 [2048, 2048], P('ep')
- attn_gain: bfloat16 [2048], replicated
- moe_gain: bfloat16 [2048], replicated
- w_gate: bfloat16 [64, 2048, 1408], P(None, 'ep')
- w_up: bfloat16 [64, 2048, 1408], P(None, 'ep')
- w_down: bfloat16 [64, 1408, 2048], P(None, None, 'ep')
- expert_ids: int32 [64, 384, 6], P(('data', 'ep')), parts along dimension 0
- slot_ids: int32 [64, 384, 6], P(('data', 'ep')), parts along dimension 0
- fill_counts: int32 [64, 64], P(('data', 'ep')), parts along dimension 0
- route_weight: bfloat16 [64, 384, 6], P(('data', 'ep')), parts along dimension 0
Outputs:
- output: bfloat16 [64, 384, 2048], P(('data', 'ep')), parts along dimension 0
There are 4 independent parts. The reference program is written for one: setup_inputs(seed, part) draws one part's arguments, and reference() takes and returns one part's arrays. A program takes and returns all parts, laid end to end along the dimension named above; an argument that names none is the same for every part.
All inputs are finite; a program needn't handle non-finite values.
Results may differ from the reference program's by a relative error of at most 0.02.
Values are sent between devices in bfloat16 or wider.
A program may use at most 768 MiB of HBM per device.

```python
import jax
import jax.numpy as jnp
from jax import lax

D = 2048
FF = 1408
EXPERTS = 64
TOP = 6
HEADS = 16
KV_HEADS = 4
HEAD_DIM = 128
GROUP = 16
BATCH_DEV = 1
SEQ = 384

TOKENS_DEV = BATCH_DEV * SEQ
CAPACITY = 2 * TOKENS_DEV * TOP // EXPERTS
BATCH = GROUP * BATCH_DEV


def expert_stack(stack_key, rows, cols, scale):
    def one_expert(expert_key):
        return (jax.random.normal(expert_key, (rows, cols), jnp.float32) * scale).astype(jnp.bfloat16)
    return lax.map(one_expert, jax.random.split(stack_key, EXPERTS))


def draw_routing(route_key):
    bias_key, hot_key, noise_key, cap_key = jax.random.split(route_key, 4)
    expert_bias = jax.random.randint(bias_key, (EXPERTS,), 0, EXPERTS)
    hot_expert = jax.random.randint(hot_key, (), 0, EXPERTS)
    is_hot = jnp.arange(EXPERTS) == hot_expert
    noise = jax.random.randint(noise_key, (GROUP, TOKENS_DEV, EXPERTS), 0, 2 * EXPERTS)
    scores = (expert_bias + jnp.where(is_hot, 4 * EXPERTS, 0) + noise) * EXPERTS + jnp.arange(EXPERTS)
    picked = lax.top_k(scores, TOP)[1]
    onehot = (picked.reshape(GROUP, TOKENS_DEV * TOP, 1) == jnp.arange(EXPERTS)).astype(jnp.int32)
    prior_hits = jnp.cumsum(onehot, axis=1) - onehot
    slot_ids = jnp.sum(prior_hits * onehot, axis=-1)
    demand = jnp.sum(onehot, axis=1)
    cap_draw = jax.random.randint(cap_key, (GROUP, EXPERTS), CAPACITY // 2, CAPACITY + 1)
    fill_counts = jnp.minimum(demand, jnp.where(is_hot, CAPACITY, cap_draw))
    return (picked.reshape(BATCH, SEQ, TOP).astype(jnp.int32), slot_ids.reshape(BATCH, SEQ, TOP).astype(jnp.int32), fill_counts.astype(jnp.int32))


def setup_inputs(seed: int = 0, part: int = 0) -> dict:
    root_key = jax.random.key(seed)
    weight_keys = jax.random.split(root_key, 8)
    part_keys = jax.random.split(jax.random.fold_in(root_key, part), 3)
    x_in = jax.random.normal(part_keys[0], (BATCH, SEQ, D), jnp.float32).astype(jnp.bfloat16)
    w_query = (jax.random.normal(weight_keys[0], (D, HEADS, HEAD_DIM), jnp.float32) * (2.0 * D ** -0.5)).astype(jnp.bfloat16)
    w_keyval = (jax.random.normal(weight_keys[1], (D, 2 * KV_HEADS, HEAD_DIM), jnp.float32) * (2.0 * D ** -0.5)).astype(jnp.bfloat16)
    w_out = (jax.random.normal(weight_keys[2], (HEADS * HEAD_DIM, D), jnp.float32) * (HEADS * HEAD_DIM) ** -0.5).astype(jnp.bfloat16)
    attn_gain = jax.random.uniform(weight_keys[3], (D,), jnp.float32, 0.5, 1.5).astype(jnp.bfloat16)
    moe_gain = jax.random.uniform(weight_keys[4], (D,), jnp.float32, 0.5, 1.5).astype(jnp.bfloat16)
    w_gate = expert_stack(weight_keys[5], D, FF, D ** -0.5)
    w_up = expert_stack(weight_keys[6], D, FF, D ** -0.5)
    w_down = expert_stack(weight_keys[7], FF, D, 2.0 * FF ** -0.5)
    expert_ids, slot_ids, fill_counts = draw_routing(part_keys[1])
    route_weight = jax.random.uniform(part_keys[2], (BATCH, SEQ, TOP), jnp.float32, 0.25, 1.0).astype(jnp.bfloat16)
    return {'x_in': x_in, 'w_query': w_query, 'w_keyval': w_keyval, 'w_out': w_out, 'attn_gain': attn_gain, 'moe_gain': moe_gain, 'w_gate': w_gate, 'w_up': w_up, 'w_down': w_down, 'expert_ids': expert_ids, 'slot_ids': slot_ids, 'fill_counts': fill_counts, 'route_weight': route_weight}


def rms_norm(val, gain):
    v32 = val.astype(jnp.float32)
    scale = lax.rsqrt(jnp.mean(v32 * v32, axis=-1, keepdims=True) + 1e-6)
    return (v32 * scale * gain.astype(jnp.float32)).astype(jnp.bfloat16)


def rotary(vals, cos_tab, sin_tab):
    half_dim = vals.shape[-1] // 2
    v32 = vals.astype(jnp.float32)
    first = v32[..., :half_dim]
    second = v32[..., half_dim:]
    return jnp.concatenate([first * cos_tab - second * sin_tab, second * cos_tab + first * sin_tab], axis=-1).astype(jnp.bfloat16)


def attend_sequence(x_row, w_query, w_keyval, w_out, attn_gain):
    groups = HEADS // KV_HEADS
    half_dim = HEAD_DIM // 2
    normed = rms_norm(x_row, attn_gain)
    query = jnp.dot(normed, w_query.reshape(D, HEADS * HEAD_DIM), preferred_element_type=jnp.float32).astype(jnp.bfloat16).reshape(SEQ, HEADS, HEAD_DIM)
    keyval = jnp.dot(normed, w_keyval.reshape(D, 2 * KV_HEADS * HEAD_DIM), preferred_element_type=jnp.float32).astype(jnp.bfloat16).reshape(SEQ, 2 * KV_HEADS, HEAD_DIM)
    inv_freq = 10000.0 ** (-jnp.arange(half_dim, dtype=jnp.float32) / half_dim)
    angles = jnp.arange(SEQ, dtype=jnp.float32)[:, None] * inv_freq[None, :]
    cos_tab = jnp.cos(angles)[:, None, :]
    sin_tab = jnp.sin(angles)[:, None, :]
    query = rotary(query, cos_tab, sin_tab).reshape(SEQ, KV_HEADS, groups, HEAD_DIM)
    keys = rotary(keyval[:, :KV_HEADS], cos_tab, sin_tab)
    values = keyval[:, KV_HEADS:]
    scores = jnp.einsum('qhgk,shk->hgqs', query.astype(jnp.float32), keys.astype(jnp.float32)) * (HEAD_DIM ** -0.5)
    causal = jnp.arange(SEQ)[:, None] >= jnp.arange(SEQ)[None, :]
    scores = jnp.where(causal, scores, -1e30)
    attn_prob = jax.nn.softmax(scores, axis=-1).astype(jnp.bfloat16)
    mixed = jnp.einsum('hgqs,shk->qhgk', attn_prob.astype(jnp.float32), values.astype(jnp.float32)).astype(jnp.bfloat16).reshape(SEQ, HEADS * HEAD_DIM)
    attn_out = jnp.dot(mixed, w_out, preferred_element_type=jnp.float32)
    return (x_row.astype(jnp.float32) + attn_out).astype(jnp.bfloat16)


def reference(x_in, w_query, w_keyval, w_out, attn_gain, moe_gain, w_gate, w_up, w_down, expert_ids, slot_ids, fill_counts, route_weight):
    hidden = lax.map(lambda seq_row: attend_sequence(seq_row, w_query, w_keyval, w_out, attn_gain), x_in)
    h_src = hidden.reshape(GROUP, TOKENS_DEV, D)
    u_src = rms_norm(h_src, moe_gain)
    u_pad = jnp.concatenate([u_src, jnp.zeros((GROUP, 1, D), jnp.bfloat16)], axis=1)
    expert_flat = expert_ids.reshape(GROUP, TOKENS_DEV * TOP)
    slot_flat = slot_ids.reshape(GROUP, TOKENS_DEV * TOP)
    weight_flat = route_weight.reshape(GROUP, TOKENS_DEV * TOP).astype(jnp.float32)
    count_at = jnp.take_along_axis(fill_counts, expert_flat, axis=1)
    flat_pos = jnp.where(slot_flat < count_at, expert_flat * CAPACITY + slot_flat, EXPERTS * CAPACITY)
    sources = jnp.arange(GROUP)[:, None]
    tok_ids = jnp.broadcast_to(jnp.arange(TOKENS_DEV * TOP, dtype=jnp.int32) // TOP, (GROUP, TOKENS_DEV * TOP))
    slot_owner = jnp.full((GROUP, EXPERTS * CAPACITY + 1), TOKENS_DEV, jnp.int32).at[sources, flat_pos].set(tok_ids)
    slot_gate = jnp.zeros((GROUP, EXPERTS * CAPACITY + 1), jnp.float32).at[sources, flat_pos].set(weight_flat)
    slot_owner = slot_owner[:, :EXPERTS * CAPACITY].reshape(GROUP, EXPERTS, CAPACITY).transpose(1, 0, 2)
    slot_gate = slot_gate[:, :EXPERTS * CAPACITY].reshape(GROUP, EXPERTS, CAPACITY).transpose(1, 0, 2)

    def expert_step(combined, block):
        gate_mat, up_mat, down_mat, rows_owner, rows_gate = block
        in_rows = u_pad[sources, rows_owner].reshape(GROUP * CAPACITY, D)
        act_gate = jnp.dot(in_rows, gate_mat, preferred_element_type=jnp.float32)
        act_up = jnp.dot(in_rows, up_mat, preferred_element_type=jnp.float32)
        hidden_mid = (jax.nn.silu(act_gate) * act_up).astype(jnp.bfloat16)
        y_rows = jnp.dot(hidden_mid, down_mat, preferred_element_type=jnp.float32).astype(jnp.bfloat16).reshape(GROUP, CAPACITY, D)
        combined = combined.at[sources, rows_owner].add(rows_gate[..., None] * y_rows.astype(jnp.float32))
        return combined, None

    start_acc = jnp.zeros((GROUP, TOKENS_DEV + 1, D), jnp.float32)
    combined = lax.scan(expert_step, start_acc, (w_gate, w_up, w_down, slot_owner, slot_gate))[0]
    out = (h_src.astype(jnp.float32) + combined[:, :TOKENS_DEV]).astype(jnp.bfloat16)
    return out.reshape(BATCH, SEQ, D)
```

```python
import functools
import math

import jax
import jax.numpy as jnp
from jax import lax
from jax.experimental import pallas as pl
from jax.experimental.pallas import tpu as pltpu
from jax.sharding import PartitionSpec as P

MESH = pl.DeviceIdType.MESH


def rms_norm(val, gain):
    v32 = val.astype(jnp.float32)
    scale = lax.rsqrt(jnp.mean(v32 * v32, axis=-1, keepdims=True) + 1e-6)
    return (v32 * scale * gain.astype(jnp.float32)).astype(jnp.bfloat16)


def rotary(vals, cos_tab, sin_tab):
    half_dim = vals.shape[-1] // 2
    v32 = vals.astype(jnp.float32)
    first = v32[..., :half_dim]
    second = v32[..., half_dim:]
    return jnp.concatenate([first * cos_tab - second * sin_tab, second * cos_tab + first * sin_tab], axis=-1).astype(jnp.bfloat16)


def attention_block(x_in, w_query, w_keyval, w_out, attn_gain):
    batch_loc, seq_len, model_dim = x_in.shape
    num_heads, head_dim = w_query.shape[1], w_query.shape[2]
    kv_heads = w_keyval.shape[1] // 2
    groups = num_heads // kv_heads
    half_dim = head_dim // 2
    normed = rms_norm(x_in, attn_gain)
    query = jnp.einsum('bsd,dhk->bshk', normed, w_query, preferred_element_type=jnp.float32).astype(jnp.bfloat16)
    keyval = jnp.einsum('bsd,dhk->bshk', normed, w_keyval, preferred_element_type=jnp.float32).astype(jnp.bfloat16)
    inv_freq = 10000.0 ** (-jnp.arange(half_dim, dtype=jnp.float32) / half_dim)
    angles = jnp.arange(seq_len, dtype=jnp.float32)[:, None] * inv_freq[None, :]
    cos_tab = jnp.cos(angles)[None, :, None, :]
    sin_tab = jnp.sin(angles)[None, :, None, :]
    query = rotary(query, cos_tab, sin_tab).reshape(batch_loc, seq_len, kv_heads, groups, head_dim)
    keys = rotary(keyval[:, :, :kv_heads], cos_tab, sin_tab)
    values = keyval[:, :, kv_heads:]
    scores = jnp.einsum('bqhgk,bshk->bhgqs', query, keys, preferred_element_type=jnp.float32) * (head_dim ** -0.5)
    causal = jnp.arange(seq_len)[:, None] >= jnp.arange(seq_len)[None, :]
    scores = jnp.where(causal, scores, -1e30)
    attn_prob = jax.nn.softmax(scores, axis=-1).astype(jnp.bfloat16)
    mixed = jnp.einsum('bhgqs,bshk->bqhgk', attn_prob, values, preferred_element_type=jnp.float32).astype(jnp.bfloat16)
    attn_out = jnp.einsum('crg,ge->cre', mixed.reshape(batch_loc, seq_len, num_heads * head_dim), w_out, preferred_element_type=jnp.float32)
    return (x_in.astype(jnp.float32) + attn_out).astype(jnp.bfloat16)


def exchange_kernel(n_ep, side, kinds, *refs):
    n = len(kinds)
    srcs, dsts = refs[:n], refs[n:2 * n]
    stage, s1_send, s1_recv, d_send, d_recv, f_send, f_recv, loc_sem = refs[2 * n:]
    dat, me = lax.axis_index('data'), lax.axis_index('ep')
    ybit = lax.rem(dat, 2)
    xbit = lax.rem(dat // side, 2)
    dat_y = dat + 1 - 2 * ybit
    dat_x = dat + side * (1 - 2 * xbit)
    place = 2 * xbit + ybit
    place_x = 2 * (1 - xbit) + ybit
    place_y = 2 * xbit + 1 - ybit
    per_dev = dsts[0].shape[0]
    chunks = [(m, j) for m in range(n) for j in range(per_dev)]

    barrier = pltpu.get_barrier_semaphore()

    @pl.loop(1, n_ep)
    def _(k):
        pl.semaphore_signal(barrier, inc=1, device_id=(dat, lax.rem(me + k, n_ep)), device_id_type=MESH)

    pl.semaphore_signal(barrier, inc=1, device_id=(dat_x, me), device_id_type=MESH)
    pl.semaphore_signal(barrier, inc=1, device_id=(dat_y, me), device_id_type=MESH)
    pl.semaphore_wait(barrier, n_ep + 1)

    def piece(m, j, owner, where):
        if kinds[m] == 'rows':
            rows = dsts[m].shape[2] // 4
            return dsts[m].at[j, owner, pl.ds(pl.multiple_of(where * rows, rows), rows), :]
        rows, cols = dsts[m].shape[1] // 4, dsts[m].shape[2] // n_ep
        return dsts[m].at[j, pl.ds(pl.multiple_of(where * rows, rows), rows), pl.ds(pl.multiple_of(owner * cols, cols), cols)]

    def quarter(m, j, where, part=None):
        if kinds[m] == 'rows':
            rows = dsts[m].shape[2] // 4
            who = pl.ds(0, n_ep) if part is None else pl.ds(part * (n_ep // 2), n_ep // 2)
            return dsts[m].at[j, who, pl.ds(pl.multiple_of(where * rows, rows), rows), :]
        rows, cols = dsts[m].shape[1] // 4, dsts[m].shape[2]
        who = pl.ds(0, cols) if part is None else pl.ds(part * (cols // 2), cols // 2)
        return dsts[m].at[j, pl.ds(pl.multiple_of(where * rows, rows), rows), who]

    def own_src(m, j, owner):
        rows = srcs[m].shape[1] // 4
        return srcs[m].at[owner * per_dev + j, pl.ds(pl.multiple_of(place * rows, rows), rows), :]

    def first(c, k):
        m, j = chunks[c]
        to, frm = lax.rem(me + k, n_ep), lax.rem(me - k + n_ep, n_ep)
        return pltpu.make_async_remote_copy(
            src_ref=own_src(m, j, to), dst_ref=piece(m, j, me, place), send_sem=s1_send.at[c, k], recv_sem=s1_recv.at[c, k],
            device_id=(dat, to), device_id_type=MESH)

    def direct(c, axis):
        m, j = chunks[c]
        ref = quarter(m, j, place)
        return pltpu.make_async_remote_copy(
            src_ref=ref, dst_ref=ref, send_sem=d_send.at[c, axis], recv_sem=d_recv.at[c, axis],
            device_id=(dat_x if axis == 0 else dat_y, me), device_id_type=MESH)

    def forward(c, axis):
        m, j = chunks[c]
        ref = quarter(m, j, place_y if axis == 0 else place_x, part=axis)
        return pltpu.make_async_remote_copy(
            src_ref=ref, dst_ref=ref, send_sem=f_send.at[c, axis], recv_sem=f_recv.at[c, axis],
            device_id=(dat_x if axis == 0 else dat_y, me), device_id_type=MESH)

    for c in range(len(chunks)):
        @pl.loop(1, n_ep)
        def _(k):
            first(c, k).start()

    for m in range(n):
        rows, cols = srcs[m].shape[1] // 4, srcs[m].shape[2]
        buf = stage[m]
        for j in range(per_dev):
            pltpu.make_async_copy(own_src(m, j, me), buf.at[j], loc_sem.at[m, j]).start()
    for m in range(n):
        buf = stage[m]
        for j in range(per_dev):
            pltpu.make_async_copy(own_src(m, j, me), buf.at[j], loc_sem.at[m, j]).wait()
            pltpu.make_async_copy(buf.at[j], piece(m, j, me, place), loc_sem.at[m, j]).start()
    for m in range(n):
        buf = stage[m]
        for j in range(per_dev):
            pltpu.make_async_copy(buf.at[j], piece(m, j, me, place), loc_sem.at[m, j]).wait()

    def pass_on(c):
        direct(c, 0).wait_recv()
        forward(c, 1).start()
        direct(c, 1).wait_recv()
        forward(c, 0).start()

    for c in range(len(chunks)):
        @pl.loop(1, n_ep)
        def _(k):
            first(c, k).wait_recv()

        direct(c, 0).start()
        direct(c, 1).start()
        if c > 0:
            pass_on(c - 1)
    pass_on(len(chunks) - 1)
    for c in range(len(chunks)):
        for axis in range(2):
            forward(c, axis).wait_recv()
            forward(c, axis).wait_send()
            direct(c, axis).wait_send()

        @pl.loop(1, n_ep)
        def _(k):
            first(c, k).wait_send()


def exchange(mats, kinds, n_ep, side, collective_id, cost):
    per_dev = mats[0].shape[0] // n_ep
    outs, stage = [], []
    for mat, kind in zip(mats, kinds):
        _, rows, cols = mat.shape
        outs.append((per_dev, n_ep, rows, cols) if kind == 'rows' else (per_dev, rows, cols * n_ep))
        stage.append(pltpu.VMEM((per_dev, rows // 4, cols), mat.dtype))
    n_chunks = len(mats) * per_dev
    dma = pltpu.SemaphoreType.DMA
    sent = sum(m.size * m.dtype.itemsize for m in mats)
    got = pl.pallas_call(
        functools.partial(exchange_kernel, n_ep, side, kinds),
        out_shape=[jax.ShapeDtypeStruct(o, m.dtype) for o, m in zip(outs, mats)],
        in_specs=[pl.BlockSpec(memory_space=pl.ANY)] * len(mats),
        out_specs=[pl.BlockSpec(memory_space=pl.ANY)] * len(mats),
        scratch_shapes=[stage, dma((n_chunks, n_ep)), dma((n_chunks, n_ep)), dma((n_chunks, 2)), dma((n_chunks, 2)),
                        dma((n_chunks, 2)), dma((n_chunks, 2)), dma((len(mats), per_dev))],
        compiler_params=pltpu.CompilerParams(collective_id=collective_id, has_side_effects=True),
        cost_estimate=pl.CostEstimate(flops=0, bytes_accessed=cost, transcendentals=0),
        name='exchange%d' % collective_id,
    )(*mats)
    return [g.reshape(g.shape[0], -1, g.shape[-1]) for g in got]


def slot_tables(ids, slots, counts, gates, experts, capacity):
    tokens, choices = ids.shape
    flat_ids, flat_slots = ids.reshape(-1), slots.reshape(-1)
    tok = jnp.repeat(jnp.arange(tokens, dtype=jnp.int32), choices)
    by_expert = (flat_ids[:, None] == jnp.arange(experts)[None, :]).astype(jnp.bfloat16)
    at_slot = (flat_slots[:, None] == jnp.arange(capacity)[None, :]).astype(jnp.bfloat16)
    cols = jnp.stack([(tok // 16).astype(jnp.bfloat16), (tok % 16).astype(jnp.bfloat16), gates.reshape(-1)], axis=1)
    spread = (at_slot[:, None, :] * cols[:, :, None]).reshape(tokens * choices, 3 * capacity)
    table = jnp.einsum('ne,nc->ec', by_expert, spread, preferred_element_type=jnp.float32).reshape(experts, 3, capacity)
    kept = jnp.arange(capacity)[None, :] < counts.reshape(-1)[:, None]
    owner = jnp.where(kept, table[:, 0] * 16 + table[:, 1], -1.0)
    gate = jnp.where(kept, table[:, 2], 0.0)
    return jnp.stack([owner, gate], axis=1)


def solution(mesh):
    row_spec = P(('data', 'ep'))
    n_ep = mesh.shape['ep']
    side = math.isqrt(mesh.shape['data'])

    def device_step(x_in, w_query, w_keyval, w_out, attn_gain, moe_gain, w_gate, w_up, w_down, expert_ids, slot_ids, fill_counts, route_weight):
        batch_loc, seq_len, model_dim = x_in.shape
        experts = w_gate.shape[0]
        per_dev = experts // n_ep
        choices = expert_ids.shape[-1]
        tokens = batch_loc * seq_len
        capacity = 2 * tokens * choices // experts
        full_query = lax.all_gather(w_query, 'ep', axis=0, tiled=True)
        full_keyval = lax.all_gather(w_keyval, 'ep', axis=0, tiled=True)
        full_out = lax.all_gather(w_out, 'ep', axis=0, tiled=True)
        (own_gate,) = exchange([w_gate], ['rows'], n_ep, side, 1, 400_000_000)
        x_in, own_gate = lax.optimization_barrier((x_in, own_gate))

        table = slot_tables(expert_ids.reshape(tokens, choices), slot_ids.reshape(tokens, choices), fill_counts, route_weight.reshape(tokens, choices), experts, capacity)
        table = lax.all_to_all(table, 'ep', 0, 1, tiled=True).reshape(per_dev, n_ep, 2, capacity)
        owner, gate = table[:, :, 0], table[:, :, 1]
        match = owner[..., None] == jnp.arange(tokens, dtype=jnp.float32)
        pick = match.astype(jnp.bfloat16)
        mix = jnp.where(match, gate[..., None], 0.0).astype(jnp.bfloat16)

        hidden = attention_block(x_in, full_query, full_keyval, full_out, attn_gain)
        h_rows = hidden.reshape(tokens, model_dim)
        u_rows = rms_norm(h_rows, moe_gain)
        all_u = lax.all_gather(u_rows, 'ep', axis=0)
        own_up, own_down = exchange([w_up, w_down], ['rows', 'cols'], n_ep, side, 2, 800_000_000)

        in_rows = jnp.einsum('esct,std->escd', pick, all_u, preferred_element_type=jnp.float32).astype(jnp.bfloat16)
        in_rows = in_rows.reshape(per_dev, n_ep * capacity, model_dim)
        act_gate = jnp.einsum('ecd,edf->ecf', in_rows, own_gate, preferred_element_type=jnp.float32)
        act_up = jnp.einsum('ecd,edf->ecf', in_rows, own_up, preferred_element_type=jnp.float32)
        hidden_mid = (jax.nn.silu(act_gate) * act_up).astype(jnp.bfloat16)
        y_rows = jnp.einsum('ecf,efd->ecd', hidden_mid, own_down, preferred_element_type=jnp.float32).astype(jnp.bfloat16)
        y_rows = y_rows.reshape(per_dev, n_ep, capacity, model_dim)
        partial = jnp.einsum('esct,escd->std', mix, y_rows, preferred_element_type=jnp.float32)
        total = lax.psum_scatter(partial, 'ep', scatter_dimension=0, tiled=False)
        out_rows = (h_rows.astype(jnp.float32) + total).astype(jnp.bfloat16)
        return out_rows.reshape(batch_loc, seq_len, model_dim)

    in_specs = (row_spec, P('ep'), P('ep'), P('ep'), P(), P(), P(None, 'ep'), P(None, 'ep'), P(None, None, 'ep'), row_spec, row_spec, row_spec, row_spec)
    return jax.shard_map(device_step, mesh=mesh, in_specs=in_specs, out_specs=row_spec, check_vma=False)
```

```python
import functools
import math

import jax
import jax.numpy as jnp
from jax import lax
from jax.experimental import pallas as pl
from jax.experimental.pallas import tpu as pltpu
from jax.sharding import PartitionSpec as P

MESH = pl.DeviceIdType.MESH


def rms_norm(val, gain):
    v32 = val.astype(jnp.float32)
    scale = lax.rsqrt(jnp.mean(v32 * v32, axis=-1, keepdims=True) + 1e-6)
    return (v32 * scale * gain.astype(jnp.float32)).astype(jnp.bfloat16)


def rotary(vals, cos_tab, sin_tab):
    half_dim = vals.shape[-1] // 2
    v32 = vals.astype(jnp.float32)
    first = v32[..., :half_dim]
    second = v32[..., half_dim:]
    return jnp.concatenate([first * cos_tab - second * sin_tab, second * cos_tab + first * sin_tab], axis=-1).astype(jnp.bfloat16)


def attention_block(x_in, w_query, w_keyval, w_out, attn_gain):
    batch_loc, seq_len, model_dim = x_in.shape
    num_heads, head_dim = w_query.shape[1], w_query.shape[2]
    kv_heads = w_keyval.shape[1] // 2
    groups = num_heads // kv_heads
    half_dim = head_dim // 2
    normed = rms_norm(x_in, attn_gain)
    query = jnp.einsum('bsd,dhk->bshk', normed, w_query, preferred_element_type=jnp.float32).astype(jnp.bfloat16)
    keyval = jnp.einsum('bsd,dhk->bshk', normed, w_keyval, preferred_element_type=jnp.float32).astype(jnp.bfloat16)
    inv_freq = 10000.0 ** (-jnp.arange(half_dim, dtype=jnp.float32) / half_dim)
    angles = jnp.arange(seq_len, dtype=jnp.float32)[:, None] * inv_freq[None, :]
    cos_tab = jnp.cos(angles)[None, :, None, :]
    sin_tab = jnp.sin(angles)[None, :, None, :]
    query = rotary(query, cos_tab, sin_tab).reshape(batch_loc, seq_len, kv_heads, groups, head_dim)
    keys = rotary(keyval[:, :, :kv_heads], cos_tab, sin_tab)
    values = keyval[:, :, kv_heads:]
    scores = jnp.einsum('bqhgk,bshk->bhgqs', query, keys, preferred_element_type=jnp.float32) * (head_dim ** -0.5)
    causal = jnp.arange(seq_len)[:, None] >= jnp.arange(seq_len)[None, :]
    scores = jnp.where(causal, scores, -1e30)
    attn_prob = jax.nn.softmax(scores, axis=-1).astype(jnp.bfloat16)
    mixed = jnp.einsum('bhgqs,bshk->bqhgk', attn_prob, values, preferred_element_type=jnp.float32).astype(jnp.bfloat16)
    attn_out = jnp.einsum('crg,ge->cre', mixed.reshape(batch_loc, seq_len, num_heads * head_dim), w_out, preferred_element_type=jnp.float32)
    return (x_in.astype(jnp.float32) + attn_out).astype(jnp.bfloat16)


def exchange_kernel(n_ep, side, kinds, *refs):
    n = len(kinds)
    srcs, dsts = refs[:n], refs[n:2 * n]
    stage, s1_send, s1_recv, d_send, d_recv, f_send, f_recv, loc_sem = refs[2 * n:]
    dat, me = lax.axis_index('data'), lax.axis_index('ep')
    ybit = lax.rem(dat, 2)
    xbit = lax.rem(dat // side, 2)
    dat_y = dat + 1 - 2 * ybit
    dat_x = dat + side * (1 - 2 * xbit)
    place = 2 * xbit + ybit
    place_x = 2 * (1 - xbit) + ybit
    place_y = 2 * xbit + 1 - ybit
    per_dev = dsts[0].shape[0]
    chunks = [(m, j) for m in range(n) for j in range(per_dev)]
    parity = {'even': 0, 'odd': 1}

    def only(m, owner):
        if kinds[m] == 'rows':
            return lambda step: step()
        return pl.when(lax.rem(owner, 2) == parity[kinds[m]])

    barrier = pltpu.get_barrier_semaphore()

    @pl.loop(1, n_ep)
    def _(k):
        pl.semaphore_signal(barrier, inc=1, device_id=(dat, lax.rem(me + k, n_ep)), device_id_type=MESH)

    pl.semaphore_signal(barrier, inc=1, device_id=(dat_x, me), device_id_type=MESH)
    pl.semaphore_signal(barrier, inc=1, device_id=(dat_y, me), device_id_type=MESH)
    pl.semaphore_wait(barrier, n_ep + 1)

    def piece(m, j, owner, where):
        if kinds[m] == 'rows':
            rows = dsts[m].shape[2] // 4
            return dsts[m].at[j, owner, pl.ds(pl.multiple_of(where * rows, rows), rows), :]
        rows, cols = dsts[m].shape[1] // 4, srcs[m].shape[2]
        return dsts[m].at[j, pl.ds(pl.multiple_of(where * rows, rows), rows), pl.ds(pl.multiple_of(owner // 2 * cols, cols), cols)]

    def quarter(m, j, where, part=None):
        if kinds[m] == 'rows':
            rows = dsts[m].shape[2] // 4
            who = pl.ds(0, n_ep) if part is None else pl.ds(part * (n_ep // 2), n_ep // 2)
            return dsts[m].at[j, who, pl.ds(pl.multiple_of(where * rows, rows), rows), :]
        rows, cols = dsts[m].shape[1] // 4, dsts[m].shape[2]
        who = pl.ds(0, cols) if part is None else pl.ds(part * (cols // 2), cols // 2)
        return dsts[m].at[j, pl.ds(pl.multiple_of(where * rows, rows), rows), who]

    def own_src(m, j, owner):
        rows = srcs[m].shape[1] // 4
        return srcs[m].at[owner * per_dev + j, pl.ds(pl.multiple_of(place * rows, rows), rows), :]

    def first(c, k):
        m, j = chunks[c]
        to, frm = lax.rem(me + k, n_ep), lax.rem(me - k + n_ep, n_ep)
        return pltpu.make_async_remote_copy(
            src_ref=own_src(m, j, to), dst_ref=piece(m, j, me, place), send_sem=s1_send.at[c, k], recv_sem=s1_recv.at[c, k],
            device_id=(dat, to), device_id_type=MESH)

    def direct(c, axis):
        m, j = chunks[c]
        ref = quarter(m, j, place)
        return pltpu.make_async_remote_copy(
            src_ref=ref, dst_ref=ref, send_sem=d_send.at[c, axis], recv_sem=d_recv.at[c, axis],
            device_id=(dat_x if axis == 0 else dat_y, me), device_id_type=MESH)

    def forward(c, axis):
        m, j = chunks[c]
        ref = quarter(m, j, place_y if axis == 0 else place_x, part=axis)
        return pltpu.make_async_remote_copy(
            src_ref=ref, dst_ref=ref, send_sem=f_send.at[c, axis], recv_sem=f_recv.at[c, axis],
            device_id=(dat_x if axis == 0 else dat_y, me), device_id_type=MESH)

    for c in range(len(chunks)):
        @only(chunks[c][0], me)
        def _():
            @pl.loop(1, n_ep)
            def _(k):
                first(c, k).start()

    for m in range(n):
        buf = stage[m]

        @only(m, me)
        def _():
            for j in range(per_dev):
                pltpu.make_async_copy(own_src(m, j, me), buf.at[j], loc_sem.at[m, j]).start()
            for j in range(per_dev):
                pltpu.make_async_copy(own_src(m, j, me), buf.at[j], loc_sem.at[m, j]).wait()
                pltpu.make_async_copy(buf.at[j], piece(m, j, me, place), loc_sem.at[m, j]).start()
            for j in range(per_dev):
                pltpu.make_async_copy(buf.at[j], piece(m, j, me, place), loc_sem.at[m, j]).wait()

    def pass_on(c):
        direct(c, 0).wait_recv()
        forward(c, 1).start()
        direct(c, 1).wait_recv()
        forward(c, 0).start()

    for c in range(len(chunks)):
        @pl.loop(1, n_ep)
        def _(k):
            @only(chunks[c][0], me - k + n_ep)
            def _():
                first(c, k).wait_recv()

        direct(c, 0).start()
        direct(c, 1).start()
        if c > 0:
            pass_on(c - 1)
    pass_on(len(chunks) - 1)
    for c in range(len(chunks)):
        for axis in range(2):
            forward(c, axis).wait_recv()
            forward(c, axis).wait_send()
            direct(c, axis).wait_send()

        @only(chunks[c][0], me)
        def _():
            @pl.loop(1, n_ep)
            def _(k):
                first(c, k).wait_send()


def exchange(mats, kinds, n_ep, side, collective_id, cost):
    per_dev = mats[0].shape[0] // n_ep
    outs, stage = [], []
    for mat, kind in zip(mats, kinds):
        _, rows, cols = mat.shape
        outs.append((per_dev, n_ep, rows, cols) if kind == 'rows' else (per_dev, rows, cols * n_ep // 2))
        stage.append(pltpu.VMEM((per_dev, rows // 4, cols), mat.dtype))
    n_chunks = len(mats) * per_dev
    dma = pltpu.SemaphoreType.DMA
    sent = sum(m.size * m.dtype.itemsize for m in mats)
    got = pl.pallas_call(
        functools.partial(exchange_kernel, n_ep, side, kinds),
        out_shape=[jax.ShapeDtypeStruct(o, m.dtype) for o, m in zip(outs, mats)],
        in_specs=[pl.BlockSpec(memory_space=pl.ANY)] * len(mats),
        out_specs=[pl.BlockSpec(memory_space=pl.ANY)] * len(mats),
        scratch_shapes=[stage, dma((n_chunks, n_ep)), dma((n_chunks, n_ep)), dma((n_chunks, 2)), dma((n_chunks, 2)),
                        dma((n_chunks, 2)), dma((n_chunks, 2)), dma((len(mats), per_dev))],
        compiler_params=pltpu.CompilerParams(collective_id=collective_id, has_side_effects=True),
        cost_estimate=pl.CostEstimate(flops=0, bytes_accessed=cost, transcendentals=0),
        name='exchange%d' % collective_id,
    )(*mats)
    return [g.reshape(g.shape[0], -1, g.shape[-1]) for g in got]


def slot_tables(ids, slots, counts, gates, experts, capacity):
    tokens, choices = ids.shape
    flat_ids, flat_slots = ids.reshape(-1), slots.reshape(-1)
    tok = jnp.repeat(jnp.arange(tokens, dtype=jnp.int32), choices)
    by_expert = (flat_ids[:, None] == jnp.arange(experts)[None, :]).astype(jnp.bfloat16)
    at_slot = (flat_slots[:, None] == jnp.arange(capacity)[None, :]).astype(jnp.bfloat16)
    cols = jnp.stack([(tok // 16).astype(jnp.bfloat16), (tok % 16).astype(jnp.bfloat16), gates.reshape(-1)], axis=1)
    spread = (at_slot[:, None, :] * cols[:, :, None]).reshape(tokens * choices, 3 * capacity)
    table = jnp.einsum('ne,nc->ec', by_expert, spread, preferred_element_type=jnp.float32).reshape(experts, 3, capacity)
    kept = jnp.arange(capacity)[None, :] < counts.reshape(-1)[:, None]
    owner = jnp.where(kept, table[:, 0] * 16 + table[:, 1], -1.0)
    gate = jnp.where(kept, table[:, 2], 0.0)
    return jnp.stack([owner, gate], axis=1)


def solution(mesh):
    row_spec = P(('data', 'ep'))
    n_ep = mesh.shape['ep']
    side = math.isqrt(mesh.shape['data'])

    def device_step(x_in, w_query, w_keyval, w_out, attn_gain, moe_gain, w_gate, w_up, w_down, expert_ids, slot_ids, fill_counts, route_weight):
        batch_loc, seq_len, model_dim = x_in.shape
        experts = w_gate.shape[0]
        per_dev = experts // n_ep
        choices = expert_ids.shape[-1]
        tokens = batch_loc * seq_len
        capacity = 2 * tokens * choices // experts
        full_query = lax.all_gather(w_query, 'ep', axis=0, tiled=True)
        full_keyval = lax.all_gather(w_keyval, 'ep', axis=0, tiled=True)
        full_out = lax.all_gather(w_out, 'ep', axis=0, tiled=True)
        (own_gate,) = exchange([w_gate], ['rows'], n_ep, side, 1, 400_000_000)
        x_in, own_gate = lax.optimization_barrier((x_in, own_gate))

        table = slot_tables(expert_ids.reshape(tokens, choices), slot_ids.reshape(tokens, choices), fill_counts, route_weight.reshape(tokens, choices), experts, capacity)
        table = lax.all_to_all(table, 'ep', 0, 1, tiled=True).reshape(per_dev, n_ep, 2, capacity)
        owner, gate = table[:, :, 0], table[:, :, 1]
        match = owner[..., None] == jnp.arange(tokens, dtype=jnp.float32)
        pick = match.astype(jnp.bfloat16)
        mix = jnp.where(match, gate[..., None], 0.0).astype(jnp.bfloat16)

        hidden = attention_block(x_in, full_query, full_keyval, full_out, attn_gain)
        h_rows = hidden.reshape(tokens, model_dim)
        u_rows = rms_norm(h_rows, moe_gain)
        all_u = lax.all_gather(u_rows, 'ep', axis=0)
        own_up, down_even = exchange([w_up, w_down], ['rows', 'even'], n_ep, side, 2, 600_000_000)

        in_rows = jnp.einsum('esct,std->escd', pick, all_u, preferred_element_type=jnp.float32).astype(jnp.bfloat16)
        in_rows = in_rows.reshape(per_dev, n_ep * capacity, model_dim)
        act_gate = jnp.einsum('ecd,edf->ecf', in_rows, own_gate, preferred_element_type=jnp.float32)
        act_up = jnp.einsum('ecd,edf->ecf', in_rows, own_up, preferred_element_type=jnp.float32)
        hidden_mid = (jax.nn.silu(act_gate) * act_up).astype(jnp.bfloat16)

        def weighted(down):
            y_rows = jnp.einsum('ecf,efd->ecd', hidden_mid, down, preferred_element_type=jnp.float32).astype(jnp.bfloat16)
            y_rows = y_rows.reshape(per_dev, n_ep, capacity, down.shape[-1])
            return jnp.einsum('esct,escd->std', mix, y_rows, preferred_element_type=jnp.float32)

        part_even = weighted(down_even)
        w_down, part_even = lax.optimization_barrier((w_down, part_even))
        sum_even = lax.psum_scatter(part_even, 'ep', scatter_dimension=0, tiled=False)
        (down_odd,) = exchange([w_down], ['odd'], n_ep, side, 3, 400_000_000)
        sum_odd = lax.psum_scatter(weighted(down_odd), 'ep', scatter_dimension=0, tiled=False)
        block = w_down.shape[-1]
        sums = [val.reshape(tokens, -1) for val in (sum_even, sum_odd)]
        total = jnp.concatenate([val[:, at:at + block] for at in range(0, model_dim // 2, block) for val in sums], axis=1)
        out_rows = (h_rows.astype(jnp.float32) + total).astype(jnp.bfloat16)
        return out_rows.reshape(batch_loc, seq_len, model_dim)

    in_specs = (row_spec, P('ep'), P('ep'), P('ep'), P(), P(), P(None, 'ep'), P(None, 'ep'), P(None, None, 'ep'), row_spec, row_spec, row_spec, row_spec)
    return jax.shard_map(device_step, mesh=mesh, in_specs=in_specs, out_specs=row_spec, check_vma=False)
```
